32 devices in a mesh: section: 4 (over y, x), dp: 8 (over z, core).
Axes of the slice: x: 2, y: 2, z: 4, core: 2. Of those that a mesh axis runs over, the one named last changes fastest.
Arguments:
- hidden_in: bfloat16 [2, 4, 4, 128, 4096], P(None, 'section', None, 'dp'), may hold values from -6 to 6
- out_grad: bfloat16 [4, 128, 4096], P(None, 'dp'), may hold values from -6 to 6
- gate_probs: float32 [2, 4, 4, 128, 2], P(None, 'section', None, 'dp'), may hold values from 0.1 to 1
- expert_ids: int32 [2, 4, 4, 128, 2], P(None, 'section', None, 'dp'), may hold values from 0 to 7, all different within a row
- task_ids: int32 [4, 8], P(None, 'dp'), may hold values from 0 to 1
- task_embed: float32 [2, 256], replicated, may hold values from -5 to 5
- slot_embed: float32 [2, 4, 8, 256], P(None, 'section'), may hold values from -5 to 5
- gen_down: bfloat16 [256, 65536], P(None, 'dp'), may hold values from -0.0078125 to 0.0078125
- gen_up: bfloat16 [256, 65536], P(None, 'dp'), may hold values from -0.09375 to 0.09375
Outputs:
- d_hidden: bfloat16 [4, 4, 128, 4096], P('section', None, 'dp')
- d_gen_down: float32 [256, 65536], P(None, 'dp')
- d_gen_up: float32 [256, 65536], P(None, 'dp')
- d_task_embed: float32 [2, 256], replicated
- d_slot_embed: float32 [2, 4, 8, 256], P(None, 'section')
The draws below stay inside these ranges and needn't reach their ends.
Inputs may be any that keep to these rules, and one draw needn't show every extreme that they name: `expert_ids`: the two experts of a token differ.
All inputs are finite; a program needn't handle non-finite values.
Results may differ from the reference program's by a relative error of at most 0.025.
Values may be sent and summed in bfloat16 or wider, within the bound.
A program may use at most 128 MiB of HBM per device.

```python
import math
import jax
import jax.numpy as jnp
from jax import lax

D = 4096
EXPERTS = 8
RANK = 16
COND = 256
TASKS = 2
BLOCKS = 2
TOK_DEV = 16
MICRO = 4
TOKENS = 128
N_SECTION = 4
N_DP = 8


def touch_ends(drawn, stream_key, least, top_value):
    longest = drawn.shape.index(max(drawn.shape))
    spots = []
    for shift in (0, 1):
        where = [jax.random.randint(jax.random.fold_in(stream_key, axis), (), 0, length) for axis, length in enumerate(drawn.shape)]
        where[longest] = (where[longest] + shift) % drawn.shape[longest]
        spots.append(tuple(where))
    return drawn.at[spots[0]].set(least).at[spots[1]].set(top_value)


def block_levels(own_key, shape, cuts, low, largest):
    loudness = 1.0
    for dim, shards_of in cuts:
        steps = jax.random.uniform(jax.random.fold_in(jax.random.fold_in(own_key, 6), dim), (shards_of,), jnp.float32, low / len(cuts), largest / len(cuts))
        loudness = loudness * jnp.repeat(jnp.exp(steps), shape[dim] // shards_of).reshape((-1,) + (1,) * (len(shape) - 1 - dim))
    return loudness


def different_ones(own_key, rows, count, top, lift):
    sequence = jax.random.permutation(jax.random.fold_in(own_key, 1), count)
    boost = sequence
    for power in range(3):
        boost = boost * boost // count
    boost = boost * lift // count
    lots = jax.random.randint(jax.random.fold_in(own_key, 2), (rows, count), 0, 4096) + boost
    holders = jax.random.permutation(jax.random.fold_in(own_key, 3), rows)[jnp.arange(count) % rows]
    lots = jnp.where(jnp.arange(rows)[:, None] == holders[None, :], 1 << 14, lots)
    score = lots * count + jnp.arange(count)
    return lax.top_k(score.astype(jnp.int32), top)[1].astype(jnp.int32)


def noise(rng, shape, width, reach, shards=(), held_as=jnp.bfloat16):
    values = width * jax.random.normal(rng, shape, jnp.float32)
    if shards:
        values = values * block_levels(rng, shape, shards, -0.22, 0.18)
    return jnp.clip(values, -reach, reach).astype(held_as)


def setup_inputs(seed: int = 0) -> dict:
    keys = jax.random.split(jax.random.key(seed), 10)
    return {
        "hidden_in": noise(keys[0], (BLOCKS, N_SECTION, MICRO, TOKENS, D), 1.0, 6.0, ((1, 4), (3, 8))),
        "out_grad": noise(keys[1], (MICRO, TOKENS, D), 1.0, 6.0, ((1, 8),)),
        "gate_probs": jnp.clip(jnp.exp(math.log(1.0) - 2.3025851 * jax.random.uniform(keys[2], (BLOCKS, N_SECTION, MICRO, TOKENS, 2), jnp.float32) ** block_levels(keys[2], (BLOCKS, N_SECTION, MICRO, TOKENS, 2), ((1, 4), (3, 8)), -0.2, 0.2)), 0.1, 1.0),
        "expert_ids": different_ones(keys[3], BLOCKS * N_SECTION * MICRO * TOKENS, EXPERTS, 2, 2048).reshape((BLOCKS, N_SECTION, MICRO, TOKENS, 2)),
        "task_ids": touch_ends(jax.random.randint(keys[4], (MICRO, N_DP), 0, TASKS), jax.random.fold_in(keys[4], 1), 0, TASKS - 1).astype(jnp.int32),
        "task_embed": noise(keys[5], (TASKS, COND), 1.0, 5.0, (), jnp.float32),
        "slot_embed": noise(keys[6], (BLOCKS, N_SECTION, EXPERTS, COND), 1.0, 5.0, ((1, 4),), jnp.float32),
        "gen_down": noise(keys[7], (COND, RANK * D), (COND * D // 2) ** -0.5, 0.0078125, ((1, 8),)),
        "gen_up": noise(keys[8], (COND, RANK * D), (COND * RANK) ** -0.5, 0.09375, ((1, 8),)),
    }


eps = 1e-05

def column_weights(gates, choices_ids, task_hot, experts, rank):
    expert_hot = (choices_ids[:, :, None] == jnp.arange(experts, dtype=jnp.int32)).astype(jnp.float32)
    per_expert = lax.optimization_barrier(jnp.sum(gates[:, :, None] * expert_hot, axis=1))
    table = task_hot[:, :, None] * per_expert[:, None, :]
    return jnp.repeat(table.reshape(table.shape[0], -1), rank, axis=1)

def layer_back(saved, cot_in, adapt_a, adapt_b, columns):
    values = saved.astype(jnp.float32)
    inv_rms = lax.rsqrt(lax.optimization_barrier(jnp.mean(values * values, axis=-1, keepdims=True)) + eps)
    normed_f = values * inv_rms
    normed = normed_f.astype(jnp.bfloat16)
    contract = (((1,), (1,)), ((), ()))
    low = lax.dot_general(normed, adapt_a, contract, preferred_element_type=jnp.float32)
    mixed_low = (columns * low).astype(jnp.bfloat16)
    back_low = lax.dot_general(cot_in, adapt_b, contract, preferred_element_type=jnp.float32)
    grad_low = (columns * back_low).astype(jnp.bfloat16)
    grad_norm = jnp.dot(grad_low, adapt_a, preferred_element_type=jnp.float32)
    grad_in = inv_rms * (grad_norm - normed_f * lax.optimization_barrier(jnp.mean(grad_norm * normed_f, axis=-1, keepdims=True)))
    result = (cot_in.astype(jnp.float32) + grad_in).astype(jnp.bfloat16)
    return (result, normed, mixed_low, grad_low)

def reference(hidden_in, out_grad, gate_probs, expert_ids, task_ids, task_embed, slot_embed, gen_down, gen_up):
    high = lax.Precision.HIGHEST
    combos = TASKS * EXPERTS
    pre_act = task_embed[None, None, :, None, :] + slot_embed[:, :, None, :, :]
    conditions = jax.nn.silu(pre_act).reshape(BLOCKS, N_SECTION, combos, COND)
    gen_a = jnp.einsum('jscw,wf->jscf', conditions, gen_down.astype(jnp.float32), precision=high).astype(jnp.bfloat16)
    gen_b = jnp.einsum('jscw,wf->jscf', conditions, gen_up.astype(jnp.float32), precision=high).astype(jnp.bfloat16)
    adapt_a = gen_a.reshape(BLOCKS, N_SECTION, combos * RANK, D)
    adapt_b = gen_b.reshape(BLOCKS, N_SECTION, combos * RANK, D)
    token_task = jnp.repeat(task_ids, TOK_DEV, axis=1).reshape(-1)
    task_hot = (token_task[:, None] == jnp.arange(TASKS, dtype=jnp.int32)).astype(jnp.float32)
    rows_contract = (((0,), (0,)), ((), ()))
    cot_now = out_grad.reshape(-1, D)
    grads_a = [[None] * N_SECTION for _ in range(BLOCKS)]
    grads_b = [[None] * N_SECTION for _ in range(BLOCKS)]
    hidden_out = [None] * N_SECTION
    for layer in reversed(range(BLOCKS * N_SECTION)):
        block_id, section_id = divmod(layer, N_SECTION)
        columns = column_weights(gate_probs[block_id, section_id].reshape(-1, 2), expert_ids[block_id, section_id].reshape(-1, 2), task_hot, EXPERTS, RANK)
        cot_prev = cot_now
        cot_now, normed, mixed_low, grad_low = layer_back(hidden_in[block_id, section_id].reshape(-1, D), cot_prev, adapt_a[block_id, section_id], adapt_b[block_id, section_id], columns)
        grads_a[block_id][section_id] = lax.dot_general(grad_low, normed, rows_contract, preferred_element_type=jnp.float32)
        grads_b[block_id][section_id] = lax.dot_general(mixed_low, cot_prev, rows_contract, preferred_element_type=jnp.float32)
        if block_id == 0:
            hidden_out[section_id] = cot_now.reshape(MICRO, TOKENS, D)
    grad_scale = 1.0 / (MICRO * TOKENS)
    full_a = jnp.stack([jnp.stack(line) for line in grads_a]).reshape(BLOCKS, N_SECTION, combos, RANK * D) * grad_scale
    full_b = jnp.stack([jnp.stack(line) for line in grads_b]).reshape(BLOCKS, N_SECTION, combos, RANK * D) * grad_scale
    d_gen_down = jnp.einsum('jscw,jscf->wf', conditions, full_a, precision=high)
    d_gen_up = jnp.einsum('jscw,jscf->wf', conditions, full_b, precision=high)
    d_cond = jnp.einsum('jscf,wf->jscw', full_a, gen_down.astype(jnp.float32), precision=high)
    d_cond = d_cond + jnp.einsum('jscf,wf->jscw', full_b, gen_up.astype(jnp.float32), precision=high)
    sigmoid_pre = jax.nn.sigmoid(pre_act)
    d_pre = d_cond.reshape(pre_act.shape) * sigmoid_pre * (1.0 + pre_act * (1.0 - sigmoid_pre))
    d_task = lax.optimization_barrier(jnp.sum(d_pre, axis=(0, 1, 3)))
    d_slot = lax.optimization_barrier(jnp.sum(d_pre, axis=2))
    return (jnp.stack(hidden_out), d_gen_down, d_gen_up, d_task, d_slot)
```

```python
import functools

import jax
import jax.numpy as jnp
from jax import lax
from jax.experimental import pallas as pl
from jax.experimental.pallas import tpu as pltpu
from jax.sharding import PartitionSpec as P

eps = 1e-05
MESH = pl.DeviceIdType.MESH
nt = (((1,), (1,)), ((), ()))
tn = (((0,), (0,)), ((), ()))
f32 = jnp.float32
bf = jnp.bfloat16


def backward(
    sizes,
    hid_in, grad_in, cols, cond_own, slots_own, task, gen_down, gen_up,
    hid_out, every, cond_all, slot_out, task_out,
    gens, hid, xn, inv_s, low_s, low_w, glow_s, landed, made, adapt, gpart, sibl, rland,
    slots_all, part, sums,
    gen_sem, in_sem, ag_send, ag_recv, sib_send, sib_recv, rsib_send, rsib_recv, rs_send, rs_recv,
    sec_send, sec_recv, rel_send, rel_recv, slot_send, slot_recv, sum_send, sum_recv,
):
    sections, ways, blocks, micro, tok, width, tasks, experts, per, cuts, piece = sizes
    me, d = lax.axis_index("section"), lax.axis_index("dp")
    chips = ways // 2
    z, c = d // 2, lax.rem(d, 2)
    pal = d + 1 - 2 * c
    last = chips - 1
    combos = tasks * experts
    rows = per * combos
    groups = ways // cuts
    ranks = groups * rows
    cond_width = gens.shape[1]
    chunk = min(piece, 1024)
    hop = width // 4
    tokens = micro * tok
    total = blocks * micro
    below, above = lax.rem(me + sections - 1, sections), lax.rem(me + 1, sections)
    scale = 1.0 / (micro * tok * ways)

    def remote(src, dst, send, recv, where):
        return pltpu.make_async_remote_copy(
            src_ref=src, dst_ref=dst, send_sem=send, recv_sem=recv,
            device_id=where, device_id_type=MESH,
        )

    def steps(low, high, body):
        def run(k, carry):
            body(k)
            return carry

        lax.fori_loop(low, high, run, 0)

    gen_copies = []
    for g, source in ((1, gen_up), (0, gen_down)):
        for n, at in enumerate(range(0, per * piece, chunk)):
            gen_copies.append(
                pltpu.make_async_copy(
                    source.at[:, pl.ds(at, chunk)], gens.at[g, :, pl.ds(at, chunk)], gen_sem.at[g, n]
                )
            )
            gen_copies[-1].start()
    hid_copy = pltpu.make_async_copy(hid_in, hid, in_sem.at[0])
    hid_copy.start()

    @pl.when(me == sections - 1)
    def _():
        pltpu.make_async_copy(grad_in, landed.at[pl.ds(0, micro)], in_sem.at[1]).start()

    barrier = pltpu.get_barrier_semaphore()

    def greet_dp(k):
        pl.semaphore_signal(
            barrier, inc=1, device_id={"dp": lax.rem(d + k, ways)}, device_id_type=MESH
        )

    def greet_section(k):
        pl.semaphore_signal(
            barrier, inc=1, device_id={"section": lax.rem(me + k, sections)}, device_id_type=MESH
        )

    steps(1, ways, greet_dp)
    steps(1, sections, greet_section)

    my_cut, my_group = lax.rem(d, cuts), d // cuts
    cond = cond_own[...]

    def generate(g):
        for n, at in enumerate(range(0, per * piece, chunk)):
            gen_copies[(1 - g) * (per * piece // chunk) + n].wait()
            out = jnp.dot(cond, gens[g, :, pl.ds(at, chunk)], preferred_element_type=f32).astype(bf)
            row, col = at // piece * combos, at % piece
            for b in range(blocks):
                adapt[b, g, my_cut, my_group, pl.ds(row, combos), pl.ds(col, chunk)] = out[
                    b * combos : (b + 1) * combos
                ]

    def shard(b, g, chip, core):
        dev = 2 * chip + core
        return adapt.at[b, g, lax.rem(dev, cuts), dev // cuts]

    def ag_hop(side, b, g, k, chip):
        ref = shard(b, g, chip, c)
        q = 2 * b + g
        to = d + 2 if side == 0 else d - 2
        return remote(
            ref, ref, ag_send.at[side, q, k - 1], ag_recv.at[side, q, k - 1], {"dp": to}
        )

    def ag_pal(b, g, chip, core):
        ref = shard(b, g, chip, core)
        q = 2 * b + g
        return remote(ref, ref, sib_send.at[q, chip], sib_recv.at[q, chip], {"dp": pal})

    def ag_start(b, g):
        @pl.when(z < last)
        def _():
            ag_hop(0, b, g, 1, z).start()

        @pl.when(z > 0)
        def _():
            ag_hop(1, b, g, 1, z).start()

        ag_pal(b, g, z, c).start()

    def ag_service(b, g, k):
        @pl.when(z >= k)
        def _():
            ag_hop(0, b, g, k, z - k).wait_recv()

            @pl.when((z < last) & (k < last))
            def _():
                ag_hop(0, b, g, k + 1, z - k).start()

            ag_pal(b, g, z - k, c).start()

        @pl.when(z + k <= last)
        def _():
            ag_hop(1, b, g, k, z + k).wait_recv()

            @pl.when((z > 0) & (k < last))
            def _():
                ag_hop(1, b, g, k + 1, z + k).start()

            ag_pal(b, g, z + k, c).start()

    def ag_finish(b, g):
        steps(0, chips, lambda chip: ag_pal(b, g, chip, 1 - c).wait_recv())

    def ag_drain(b, g):
        def one(k):
            @pl.when((z < last) & (z - k + 1 >= 0))
            def _():
                ag_hop(0, b, g, k, z - k + 1).wait_send()

            @pl.when((z > 0) & (z + k - 1 <= last))
            def _():
                ag_hop(1, b, g, k, z + k - 1).wait_send()

        steps(1, chips, one)
        steps(0, chips, lambda chip: ag_pal(b, g, chip, c).wait_send())

    def spans(size):
        for at in range(0, width, size):
            yield at, at // piece, at % piece

    def panel(b, g, at, size):
        return adapt[b, g, at // piece, :, :, pl.ds(at % piece, size)].reshape(ranks, size)

    def norm(b):
        square = jnp.zeros((tokens, 1), f32)
        for at, _, _ in spans(chunk):
            x = hid[b, :, pl.ds(at, chunk)].astype(f32)
            square += jnp.sum(x * x, axis=-1, keepdims=True)
        inv = lax.rsqrt(square * (1.0 / width) + eps)
        inv_s[b] = inv
        for at, _, _ in spans(chunk):
            xn[b, :, pl.ds(at, chunk)] = (hid[b, :, pl.ds(at, chunk)].astype(f32) * inv).astype(bf)

    def project(b):
        low = jnp.zeros((tokens, ranks), f32)
        for at, _, _ in spans(chunk):
            low += lax.dot_general(
                xn[b, :, pl.ds(at, chunk)], panel(b, 0, at, chunk), nt, preferred_element_type=f32
            )
        low_s[b] = low
        low_w[b] = (cols[b] * low).astype(bf)

    def relay_hop(item, slot, n):
        at = pl.ds(n * hop, hop)
        return remote(
            made.at[item, :, at], landed.at[slot, :, at],
            rel_send.at[item, n], rel_recv.at[slot, n], {"section": below},
        )

    def relay(b):
        first_item = (blocks - 1 - b) * micro

        def one(m):
            item = first_item + m
            mine = pl.ds(pl.multiple_of(m * tok, tok), tok)
            back = jnp.zeros((tok, ranks), f32)
            for n in range(4):
                if b == blocks - 1:
                    @pl.when(me < sections - 1)
                    def _():
                        relay_hop(item, item, n).wait_recv()
                else:
                    relay_hop(item, item, n).wait_recv()
                for at in range(n * hop, (n + 1) * hop, min(hop, chunk)):
                    back += lax.dot_general(
                        landed[item, :, pl.ds(at, min(hop, chunk))], panel(b, 1, at, min(hop, chunk)),
                        nt, preferred_element_type=f32,
                    )
            glow = (cols[b, mine] * back).astype(bf)
            glow_s[b, mine] = glow
            dots = jnp.sum(glow.astype(f32) * low_s[b, mine], axis=-1, keepdims=True) * (1.0 / width)
            inv = inv_s[b, mine]
            scaled = dots * inv
            for n in range(4):
                for at in range(n * hop, (n + 1) * hop, min(hop, chunk)):
                    size = min(hop, chunk)
                    up = jnp.dot(glow, panel(b, 0, at, size), preferred_element_type=f32)
                    xf = hid[b, mine, pl.ds(at, size)].astype(f32) * inv
                    dx = landed[item, :, pl.ds(at, size)].astype(f32) + (inv * up - xf * scaled)
                    dx = dx.astype(bf)
                    made[item, :, pl.ds(at, size)] = dx
                    if b == 0:
                        hid_out[m, :, pl.ds(at, size)] = dx

                @pl.when(me > 0)
                def _():
                    relay_hop(item, item, n).start()

                if b > 0:
                    @pl.when(me == 0)
                    def _():
                        relay_hop(item, item + micro, n).start()

        steps(0, micro, one)

    def relay_drain(item):
        for n in range(4):
            @pl.when((me > 0) | (item < total - micro))
            def _():
                relay_hop(item, item, n).wait_send()

    def grads(b, g):
        base = (blocks - 1 - b) * micro
        left = (glow_s if g == 0 else low_w)[b]
        for at, cut, col in spans(chunk):
            if g == 0:
                right = xn[b, :, pl.ds(at, chunk)]
            else:
                right = landed[pl.ds(base, micro), :, pl.ds(at, chunk)].reshape(tokens, chunk)
            out = lax.dot_general(left, right, tn, preferred_element_type=f32) * scale
            gpart[b, g, cut, :, :, pl.ds(col, chunk)] = out.astype(bf).reshape(groups, rows, chunk)

    def bucket(b, g, chip, core):
        dev = 2 * chip + core
        return gpart.at[b, g, lax.rem(dev, cuts), dev // cuts]

    def rs_pal(b, g, chip, core):
        q = 2 * b + g
        return remote(
            bucket(b, g, chip, core), sibl.at[q, chip],
            rsib_send.at[q, chip], rsib_recv.at[q, chip], {"dp": pal},
        )

    def rs_hop(side, b, g, k, dest):
        q = 2 * b + g
        to = d + 2 if side == 0 else d - 2
        return remote(
            bucket(b, g, dest, c), rland.at[side, q, k - 1],
            rs_send.at[side, q, k - 1], rs_recv.at[side, q, k - 1], {"dp": to},
        )

    def add_into(target, *others):
        for at in range(0, piece, chunk):
            value = target[:, pl.ds(at, chunk)].astype(f32)
            for other in others:
                value = value + other[:, pl.ds(at, chunk)].astype(f32)
            target[:, pl.ds(at, chunk)] = value.astype(bf)

    def rs_exchange(b, g):
        steps(0, chips, lambda chip: rs_pal(b, g, chip, 1 - c).start())

    def rs_start(b, g):
        def one(chip):
            rs_pal(b, g, chip, c).wait_recv()
            add_into(bucket(b, g, chip, c), sibl.at[2 * b + g, chip])

        steps(0, chips, one)

        @pl.when(z == 0)
        def _():
            steps(1, chips, lambda k: rs_hop(0, b, g, k, chips - k).start())

        @pl.when(z == last)
        def _():
            steps(1, chips, lambda k: rs_hop(1, b, g, k, k - 1).start())

    def rs_service(b, g, k):
        q = 2 * b + g

        @pl.when((z >= 1) & (k >= z) & (k < last))
        def _():
            dest = chips - k + z - 1
            rs_hop(0, b, g, k, dest).wait_recv()
            add_into(bucket(b, g, dest, c), rland.at[0, q, k - 1])
            rs_hop(0, b, g, k + 1, dest).start()

        @pl.when((z < last) & (k >= last - z) & (k < last))
        def _():
            dest = z + k - last
            rs_hop(1, b, g, k, dest).wait_recv()
            add_into(bucket(b, g, dest, c), rland.at[1, q, k - 1])
            rs_hop(1, b, g, k + 1, dest).start()

    def rs_finish(b, g):
        q = 2 * b + g

        @pl.when(z >= 1)
        def _():
            rs_hop(0, b, g, last, z).wait_recv()

        @pl.when(z < last)
        def _():
            rs_hop(1, b, g, last, z).wait_recv()

        own = bucket(b, g, z, c)

        def put(*others):
            for at in range(0, piece, chunk):
                value = own[:, pl.ds(at, chunk)].astype(f32)
                for other in others:
                    value = value + other[:, pl.ds(at, chunk)].astype(f32)
                every[me, b, g, :, pl.ds(at, chunk)] = value.astype(bf)

        @pl.when(z == 0)
        def _():
            put(rland.at[1, q, last - 1])

        @pl.when(z == last)
        def _():
            put(rland.at[0, q, last - 1])

        @pl.when((z > 0) & (z < last))
        def _():
            put(rland.at[0, q, last - 1], rland.at[1, q, last - 1])

    def rs_drain(b, g):
        steps(0, chips, lambda chip: rs_pal(b, g, chip, 1 - c).wait_send())

        def one(k):
            @pl.when(k >= z + 1)
            def _():
                rs_hop(0, b, g, k, chips - k + z).wait_send()

            @pl.when(k >= chips - z)
            def _():
                rs_hop(1, b, g, k, k - chips + z).wait_send()

        steps(1, chips, one)

    def sec_hop(b, g, k, owner):
        q = 2 * b + g
        ref = every.at[owner, b, g]
        return remote(
            ref, ref, sec_send.at[q, k - 1], sec_recv.at[q, k - 1],
            {"section": lax.rem(me + k, sections)},
        )

    def sec_start(b, g):
        for k in range(1, sections):
            sec_hop(b, g, k, me).start()

    def sec_finish(b, g):
        for k in range(1, sections):
            sec_hop(b, g, k, lax.rem(me + sections - k, sections)).wait_recv()

    def sec_drain(b, g):
        for k in range(1, sections):
            sec_hop(b, g, k, me).wait_send()

    def contract(b, g):
        out = jnp.zeros((sections * combos, cond_width), f32)
        for at in range(0, per * piece, chunk):
            row, col = at // piece * combos, at % piece
            left = every[:, b, g, pl.ds(row, combos), pl.ds(col, chunk)]
            out += lax.dot_general(
                left.reshape(sections * combos, chunk), gens[g, :, pl.ds(at, chunk)], nt,
                preferred_element_type=f32,
            )
        part[:, b] += out.reshape(sections, combos, cond_width)

    def slot_hop(k, owner):
        ref = slots_all.at[owner]
        return remote(
            slots_own, ref, slot_send.at[k - 1], slot_recv.at[k - 1],
            {"section": lax.rem(me + k, sections)},
        )

    def sum_hop(k):
        return remote(
            sums.at[d], sums.at[d], sum_send.at[k - 1], sum_recv.at[d],
            {"dp": lax.rem(d + k, ways)},
        )

    top, kinds = blocks - 1, (1, 0)
    generate(1)
    pl.semaphore_wait(barrier, ways - 1 + sections - 1)
    ag_start(top, 1)
    generate(0)
    ag_start(top, 0)
    for k in range(1, sections):
        slot_hop(k, me).start()
    hid_copy.wait()
    for b in reversed(range(blocks)):
        norm(b)
    part[...] = jnp.zeros_like(part)

    def both(fn, *args):
        for g in kinds:
            fn(*args[:1], g, *args[1:])

    steps(1, chips, lambda k: both(ag_service, top, k))
    for b in reversed(range(top)):
        both(ag_start, b)
    both(ag_finish, top)
    project(top)

    @pl.when(me == sections - 1)
    def _():
        pltpu.make_async_copy(grad_in, landed.at[pl.ds(0, micro)], in_sem.at[1]).wait()

    for b in reversed(range(blocks)):
        if b > 0:
            early = me < sections // 2

            @pl.when(early)
            def _():
                both(ag_service, b - 1, 1)

        relay(b)
        if b > 0:
            @pl.when(jnp.logical_not(early))
            def _():
                both(ag_service, b - 1, 1)

        for g in (0, 1):
            grads(b, g)
        if b > 0:
            steps(2, last, lambda k: both(ag_service, b - 1, k))
            for g in (0, 1):
                rs_exchange(b, g)
            for g in (0, 1):
                rs_start(b, g)
            if last > 1:
                both(ag_service, b - 1, last)
            both(ag_finish, b - 1)
            project(b - 1)
        else:
            for g in (0, 1):
                rs_exchange(b, g)
        if b == top:
            continue
        for g in (0, 1):
            steps(1, last, lambda k: rs_service(b + 1, g, k))
        for g in (0, 1):
            if b == 0:
                rs_start(b, g)
        for g in (0, 1):
            rs_finish(b + 1, g)
            sec_start(b + 1, g)
    for k in range(1, sections):
        slot_hop(k, lax.rem(me + sections - k, sections)).wait_recv()
    slots_all[me] = slots_own[...]
    pre = task[...][None, None, :, None, :] + slots_all[...][:, :, None, :, :]
    sig = 1.0 / (1.0 + jnp.exp(-pre))
    cond_all[...] = (pre * sig).reshape(sections * blocks * combos, cond_width).astype(bf)
    slope = sig * (1.0 + pre * (1.0 - sig))
    for b in range(1, blocks):
        for g in (0, 1):
            sec_finish(b, g)
            contract(b, g)
    for g in (0, 1):
        steps(1, last, lambda k: rs_service(0, g, k))
        rs_finish(0, g)
        sec_start(0, g)
    for g in (0, 1):
        sec_finish(0, g)
        contract(0, g)

    d_pre = part[...].reshape(sections, blocks, tasks, experts, cond_width) * slope
    part[...] = d_pre.reshape(sections, blocks, combos, cond_width)
    own = part[me].reshape(blocks, tasks, experts, cond_width)
    sums[d] = jnp.zeros_like(sums[d])
    sums[d, pl.ds(0, blocks * experts)] = jnp.sum(own, axis=1).reshape(blocks * experts, cond_width)
    sums[d, pl.ds(blocks * experts, tasks)] = jnp.sum(d_pre, axis=(0, 1, 3))
    steps(1, ways, lambda k: sum_hop(k).start())

    for b in range(blocks):
        for g in (0, 1):
            ag_drain(b, g)
            rs_drain(b, g)
            sec_drain(b, g)
    steps(0, total, relay_drain)
    for k in range(1, sections):
        slot_hop(k, me).wait_send()

    def sum_wait(k):
        other = lax.rem(d + k, ways)
        remote(
            sums.at[other], sums.at[other], sum_send.at[k - 1], sum_recv.at[other],
            {"dp": other},
        ).wait_recv()

    steps(1, ways, sum_wait)
    steps(1, ways, lambda k: sum_hop(k).wait_send())
    whole = jnp.sum(sums[...], axis=0)
    slot_out[...] = whole[: blocks * experts]
    task_out[...] = whole[blocks * experts : blocks * experts + tasks]


def generators(cond, every, down, up):
    rows = cond.shape[0]
    for g, out in ((0, down), (1, up)):
        right = every[:, :, g].reshape(rows, every.shape[-1])
        out[...] = lax.dot_general(cond[...], right, tn, preferred_element_type=f32)


def on_device(
    hidden_in, out_grad, gate_probs, expert_ids, task_ids, task_embed, slot_embed, gen_down, gen_up
):
    sections, ways = lax.axis_size("section"), lax.axis_size("dp")
    blocks, _, micro, tok, width = hidden_in.shape
    tasks, cond_width = task_embed.shape
    experts = slot_embed.shape[2]
    combos = tasks * experts
    span = gen_down.shape[1]
    per = max(1, span // width)
    cuts = max(1, width // span)
    piece = span // per
    rows = per * combos
    groups = ways // cuts
    ranks = groups * rows
    total, tokens, chips = blocks * micro, micro * tok, ways // 2
    quads = 2 * blocks
    chunk = min(piece, 1024)

    slots_own = slot_embed[:, 0]
    pre_own = task_embed[None, :, None, :] + slots_own[:, None, :, :]
    cond_own = jax.nn.silu(pre_own).reshape(-1, cond_width).astype(bf)
    hot = (expert_ids[:, 0][..., None] == jnp.arange(experts, dtype=jnp.int32)).astype(f32)
    per_expert = jnp.sum(gate_probs[:, 0][..., None] * hot, axis=3)
    task_hot = (task_ids == jnp.arange(tasks, dtype=jnp.int32)).astype(f32)
    table = task_hot[None, :, None, :, None] * per_expert[:, :, :, None, :]
    cols = jnp.tile(table.reshape(blocks, tokens, combos), (1, 1, ranks // combos))

    vmem = pl.BlockSpec(memory_space=pltpu.VMEM)
    anywhere = pl.BlockSpec(memory_space=pl.ANY)
    sem = pltpu.SemaphoreType.DMA
    sizes = (sections, ways, blocks, micro, tok, width, tasks, experts, per, cuts, piece)
    hid_out, every, cond_all, d_slot, d_task = pl.pallas_call(
        functools.partial(backward, sizes),
        out_shape=(
            jax.ShapeDtypeStruct((micro, tok, width), bf),
            jax.ShapeDtypeStruct((sections, blocks, 2, rows, piece), bf),
            jax.ShapeDtypeStruct((sections * blocks * combos, cond_width), bf),
            jax.ShapeDtypeStruct((blocks * experts, cond_width), f32),
            jax.ShapeDtypeStruct((tasks, cond_width), f32),
        ),
        in_specs=[anywhere, anywhere, vmem, vmem, vmem, vmem, anywhere, anywhere],
        out_specs=(vmem,) * 5,
        scratch_shapes=[
            pltpu.VMEM((2, cond_width, span), bf),
            pltpu.VMEM((blocks, tokens, width), bf),
            pltpu.VMEM((blocks, tokens, width), bf),
            pltpu.VMEM((blocks, tokens, 1), f32),
            pltpu.VMEM((blocks, tokens, ranks), f32),
            pltpu.VMEM((blocks, tokens, ranks), bf),
            pltpu.VMEM((blocks, tokens, ranks), bf),
            pltpu.VMEM((total, tok, width), bf),
            pltpu.VMEM((total, tok, width), bf),
            pltpu.VMEM((blocks, 2, cuts, groups, rows, piece), bf),
            pltpu.VMEM((blocks, 2, cuts, groups, rows, piece), bf),
            pltpu.VMEM((quads, chips, rows, piece), bf),
            pltpu.VMEM((2, quads, chips - 1, rows, piece), bf),
            pltpu.VMEM((sections, blocks, experts, cond_width), f32),
            pltpu.VMEM((sections, blocks, combos, cond_width), f32),
            pltpu.VMEM((ways, blocks * experts + 8, cond_width), f32),
            sem((2, span // chunk)),
            sem((2,)),
            sem((2, quads, chips - 1)),
            sem((2, quads, chips - 1)),
            sem((quads, chips)),
            sem((quads, chips)),
            sem((quads, chips)),
            sem((quads, chips)),
            sem((2, quads, chips - 1)),
            sem((2, quads, chips - 1)),
            sem((quads, sections - 1)),
            sem((quads, sections - 1)),
            sem((total, 4)),
            sem((total, 4)),
            sem((sections - 1,)),
            sem((sections - 1,)),
            sem((ways - 1,)),
            sem((ways,)),
        ],
        compiler_params=pltpu.CompilerParams(
            collective_id=1, has_side_effects=True, vmem_limit_bytes=58 << 20
        ),
        name="backward",
    )(
        hidden_in.reshape(blocks, tokens, width), out_grad, cols, cond_own, slots_own, task_embed,
        gen_down, gen_up,
    )

    out_chunk = min(piece, 1024)
    d_down, d_up = pl.pallas_call(
        generators,
        grid=(per, piece // out_chunk),
        out_shape=(jax.ShapeDtypeStruct((cond_width, span), f32),) * 2,
        in_specs=[
            pl.BlockSpec((sections * blocks * combos, cond_width), lambda p, i: (0, 0)),
            pl.BlockSpec((sections, blocks, 2, combos, out_chunk), lambda p, i: (0, 0, 0, p, i)),
        ],
        out_specs=(
            pl.BlockSpec((cond_width, out_chunk), lambda p, i: (0, p * (piece // out_chunk) + i)),
        ) * 2,
        compiler_params=pltpu.CompilerParams(vmem_limit_bytes=24 << 20),
        name="generators",
    )(cond_all, every)
    return (
        hid_out[None], d_down, d_up, d_task,
        d_slot.reshape(blocks, 1, experts, cond_width),
    )


def solution(mesh):
    placed = (
        P(None, "section", None, "dp", None),
        P(None, "dp", None),
        P(None, "section", None, "dp", None),
        P(None, "section", None, "dp", None),
        P(None, "dp"),
        P(),
        P(None, "section", None, None),
        P(None, "dp"),
        P(None, "dp"),
    )
    return jax.shard_map(
        on_device,
        mesh=mesh,
        in_specs=placed,
        out_specs=(
            P("section", None, "dp", None),
            P(None, "dp"),
            P(None, "dp"),
            P(),
            P(None, "section", None, None),
        ),
        check_vma=False,
    )
```

```python
import functools

import jax
import jax.numpy as jnp
from jax import lax
from jax.experimental import pallas as pl
from jax.experimental.pallas import tpu as pltpu
from jax.sharding import PartitionSpec as P

eps = 1e-05
MESH = pl.DeviceIdType.MESH
nt = (((1,), (1,)), ((), ()))
tn = (((0,), (0,)), ((), ()))
f32 = jnp.float32
bf = jnp.bfloat16


def backward(
    sizes,
    hid_in, grad_in, gates, picks, task_ids, slots_own, task, gen_down, gen_up,
    hid_out, every, cond_all, slot_out, task_out,
    gens, hid, xn, inv_s, low_s, low_w, glow_s, landed, made, adapt, gpart, sibl, rland,
    cols, reduced, slots_all, part, sums,
    gen_sem, in_sem, out_sem, put_sem, ag_send, ag_recv, sib_send, sib_recv, rsib_send, rsib_recv, rs_send, rs_recv,
    sec_send, sec_recv, rel_send, rel_recv, slot_send, slot_recv, sum_send, sum_recv,
    task_send, task_recv,
):
    sections, ways, blocks, micro, tok, width, tasks, experts, per, cuts, piece = sizes
    me, d = lax.axis_index("section"), lax.axis_index("dp")
    chips = ways // 2
    z, c = d // 2, lax.rem(d, 2)
    pal = d + 1 - 2 * c
    last = chips - 1
    combos = tasks * experts
    rows = per * combos
    groups = ways // cuts
    ranks = groups * rows
    cond_width = gens.shape[1]
    chunk = min(piece, 1024)
    hop = width // 4
    parts = rland.shape[1] // (2 * blocks)
    sub = piece // parts
    strip = min(sub, 1024)
    tokens = micro * tok
    total = blocks * micro
    below, above = lax.rem(me + sections - 1, sections), lax.rem(me + 1, sections)
    scale = 1.0 / (micro * tok * ways)

    def remote(src, dst, send, recv, where):
        return pltpu.make_async_remote_copy(
            src_ref=src, dst_ref=dst, send_sem=send, recv_sem=recv,
            device_id=where, device_id_type=MESH,
        )

    def steps(low, high, body):
        def run(k, carry):
            body(k)
            return carry

        lax.fori_loop(low, high, run, 0)

    gen_copies = []
    for g, source in ((1, gen_up), (0, gen_down)):
        for n, at in enumerate(range(0, per * piece, chunk)):
            gen_copies.append(
                pltpu.make_async_copy(
                    source.at[:, pl.ds(at, chunk)], gens.at[g, :, pl.ds(at, chunk)], gen_sem.at[g, n]
                )
            )
            gen_copies[-1].start()
    hid_copy = pltpu.make_async_copy(hid_in, hid, in_sem.at[0])
    hid_copy.start()

    @pl.when(me == sections - 1)
    def _():
        pltpu.make_async_copy(grad_in, landed.at[pl.ds(0, micro)], in_sem.at[1]).start()

    barrier = pltpu.get_barrier_semaphore()

    def greet_dp(k):
        pl.semaphore_signal(
            barrier, inc=1, device_id={"dp": lax.rem(d + k, ways)}, device_id_type=MESH
        )

    def greet_section(k):
        pl.semaphore_signal(
            barrier, inc=1, device_id={"section": lax.rem(me + k, sections)}, device_id_type=MESH
        )

    steps(1, ways, greet_dp)
    steps(1, sections, greet_section)

    my_cut, my_group = lax.rem(d, cuts), d // cuts
    pre = task[...][None, :, None, :] + slots_own[...][:, None, :, :]
    sig = 1.0 / (1.0 + jnp.exp(-pre))
    cond = (pre * sig).reshape(blocks * combos, cond_width).astype(bf)

    def weigh():
        eye = lax.broadcasted_iota(jnp.int32, (tok, tok), 0) == lax.broadcasted_iota(
            jnp.int32, (tok, tok), 1
        )
        lane = lax.broadcasted_iota(jnp.int32, (tok, ranks), 1)
        expert = lax.rem(lane, experts).astype(f32)
        task_of = lax.rem(lane, combos) // experts

        def column(row):
            return jnp.sum(jnp.where(eye, row, 0.0), axis=1, keepdims=True)

        for m in range(micro):
            right_task = jnp.where(task_of == task_ids[m, 0], 1.0, 0.0)
            for b in range(blocks):
                total_weight = jnp.zeros((tok, ranks), f32)
                for k in range(gates.shape[2]):
                    pick = column(picks[b, m, k : k + 1].astype(f32))
                    gate = column(gates[b, m, k : k + 1])
                    total_weight += jnp.where(pick == expert, gate, 0.0)
                cols[b, m * tok : (m + 1) * tok] = right_task * total_weight

    def generate(g):
        for n, at in enumerate(range(0, per * piece, chunk)):
            gen_copies[(1 - g) * (per * piece // chunk) + n].wait()
            out = jnp.dot(cond, gens[g, :, pl.ds(at, chunk)], preferred_element_type=f32).astype(bf)
            row, col = at // piece * combos, at % piece
            for b in range(blocks):
                adapt[b, g, my_cut, my_group, pl.ds(row, combos), pl.ds(col, chunk)] = out[
                    b * combos : (b + 1) * combos
                ]

    def shard(b, g, chip, core):
        dev = 2 * chip + core
        return adapt.at[b, g, lax.rem(dev, cuts), dev // cuts]

    def ag_hop(side, b, g, k, chip):
        ref = shard(b, g, chip, c)
        q = 2 * b + g
        to = d + 2 if side == 0 else d - 2
        return remote(
            ref, ref, ag_send.at[side, q, k - 1], ag_recv.at[side, q, k - 1], {"dp": to}
        )

    def ag_pal(b, g, chip, core):
        ref = shard(b, g, chip, core)
        q = 2 * b + g
        return remote(ref, ref, sib_send.at[q, chip], sib_recv.at[q, chip], {"dp": pal})

    def ag_start(b, g):
        @pl.when(z < last)
        def _():
            ag_hop(0, b, g, 1, z).start()

        @pl.when(z > 0)
        def _():
            ag_hop(1, b, g, 1, z).start()

        ag_pal(b, g, z, c).start()

    def ag_service(b, g, k):
        @pl.when(z >= k)
        def _():
            ag_hop(0, b, g, k, z - k).wait_recv()

            @pl.when((z < last) & (k < last))
            def _():
                ag_hop(0, b, g, k + 1, z - k).start()

            ag_pal(b, g, z - k, c).start()

        @pl.when(z + k <= last)
        def _():
            ag_hop(1, b, g, k, z + k).wait_recv()

            @pl.when((z > 0) & (k < last))
            def _():
                ag_hop(1, b, g, k + 1, z + k).start()

            ag_pal(b, g, z + k, c).start()

    def ag_finish(b, g):
        steps(0, chips, lambda chip: ag_pal(b, g, chip, 1 - c).wait_recv())

    def ag_drain(b, g):
        def one(k):
            @pl.when((z < last) & (z - k + 1 >= 0))
            def _():
                ag_hop(0, b, g, k, z - k + 1).wait_send()

            @pl.when((z > 0) & (z + k - 1 <= last))
            def _():
                ag_hop(1, b, g, k, z + k - 1).wait_send()

        steps(1, chips, one)
        steps(0, chips, lambda chip: ag_pal(b, g, chip, c).wait_send())

    def spans(size):
        for at in range(0, width, size):
            yield at, at // piece, at % piece

    def panel(b, g, at, size):
        return adapt[b, g, at // piece, :, :, pl.ds(at % piece, size)].reshape(ranks, size)

    def norm(b):
        square = jnp.zeros((tokens, 1), f32)
        for at, _, _ in spans(chunk):
            x = hid[b, :, pl.ds(at, chunk)].astype(f32)
            square += jnp.sum(x * x, axis=-1, keepdims=True)
        inv = lax.rsqrt(square * (1.0 / width) + eps)
        inv_s[b] = inv
        for at, _, _ in spans(chunk):
            xn[b, :, pl.ds(at, chunk)] = (hid[b, :, pl.ds(at, chunk)].astype(f32) * inv).astype(bf)

    def project(b):
        low = jnp.zeros((tokens, ranks), f32)
        for at, _, _ in spans(chunk):
            low += lax.dot_general(
                xn[b, :, pl.ds(at, chunk)], panel(b, 0, at, chunk), nt, preferred_element_type=f32
            )
        low_s[b] = low
        low_w[b] = (cols[b] * low).astype(bf)

    def relay_hop(item, slot, n):
        at = pl.ds(n * hop, hop)
        return remote(
            made.at[item, :, at], landed.at[slot, :, at],
            rel_send.at[item, n], rel_recv.at[slot, n], {"section": below},
        )

    def hid_put(m):
        return pltpu.make_async_copy(
            made.at[total - micro + m], hid_out.at[m], out_sem.at[m]
        )

    def relay(b, between):
        first_item = (blocks - 1 - b) * micro

        def one(m):
            item = first_item + m
            between(m)
            mine = pl.ds(pl.multiple_of(m * tok, tok), tok)
            back = jnp.zeros((tok, ranks), f32)
            for n in range(4):
                if b == blocks - 1:
                    @pl.when(me < sections - 1)
                    def _():
                        relay_hop(item, item, n).wait_recv()
                else:
                    relay_hop(item, item, n).wait_recv()
                for at in range(n * hop, (n + 1) * hop, min(hop, chunk)):
                    back += lax.dot_general(
                        landed[item, :, pl.ds(at, min(hop, chunk))], panel(b, 1, at, min(hop, chunk)),
                        nt, preferred_element_type=f32,
                    )
            glow = (cols[b, mine] * back).astype(bf)
            glow_s[b, mine] = glow
            dots = jnp.sum(glow.astype(f32) * low_s[b, mine], axis=-1, keepdims=True) * (1.0 / width)
            inv = inv_s[b, mine]
            scaled = dots * inv
            for n in range(4):
                for at in range(n * hop, (n + 1) * hop, min(hop, chunk)):
                    size = min(hop, chunk)
                    up = jnp.dot(glow, panel(b, 0, at, size), preferred_element_type=f32)
                    xf = hid[b, mine, pl.ds(at, size)].astype(f32) * inv
                    dx = landed[item, :, pl.ds(at, size)].astype(f32) + (inv * up - xf * scaled)
                    dx = dx.astype(bf)
                    made[item, :, pl.ds(at, size)] = dx

                @pl.when(me > 0)
                def _():
                    relay_hop(item, item, n).start()

                if b > 0:
                    @pl.when(me == 0)
                    def _():
                        relay_hop(item, item + micro, n).start()

            if b == 0:
                hid_put(m).start()

        steps(0, micro, one)

    def relay_drain(item):
        for n in range(4):
            @pl.when((me > 0) | (item < total - micro))
            def _():
                relay_hop(item, item, n).wait_send()

    def grads(b, g):
        base = (blocks - 1 - b) * micro
        left = (glow_s if g == 0 else low_w)[b]
        for at, cut, col in spans(chunk):
            if g == 0:
                right = xn[b, :, pl.ds(at, chunk)]
            else:
                right = landed[pl.ds(base, micro), :, pl.ds(at, chunk)].reshape(tokens, chunk)
            out = lax.dot_general(left, right, tn, preferred_element_type=f32) * scale
            gpart[b, g, cut, :, :, pl.ds(col, chunk)] = out.astype(bf).reshape(groups, rows, chunk)

    def bucket(b, g, h, chip, core):
        dev = 2 * chip + core
        return gpart.at[b, g, lax.rem(dev, cuts), dev // cuts, :, pl.ds(h * sub, sub)]

    def number(b, g, h):
        return (2 * b + g) * parts + h

    def rs_pal(b, g, h, chip, core):
        q = number(b, g, h)
        return remote(
            bucket(b, g, h, chip, core), sibl.at[q, chip],
            rsib_send.at[q, chip], rsib_recv.at[q, chip], {"dp": pal},
        )

    def rs_hop(side, b, g, h, k, dest):
        q = number(b, g, h)
        to = d + 2 if side == 0 else d - 2
        return remote(
            bucket(b, g, h, dest, c), rland.at[side, q, k - 1],
            rs_send.at[side, q, k - 1], rs_recv.at[side, q, k - 1], {"dp": to},
        )

    def add_into(target, *others):
        for at in range(0, sub, strip):
            value = target[:, pl.ds(at, strip)].astype(f32)
            for other in others:
                value = value + other[:, pl.ds(at, strip)].astype(f32)
            target[:, pl.ds(at, strip)] = value.astype(bf)

    def nth(n):
        return jnp.where(2 * z < chips, last - n, n)

    def rs_exchange(b, g):
        for h in range(parts):
            steps(0, chips, lambda n: rs_pal(b, g, h, nth(n), 1 - c).start())

    def rs_start(b, g, h):
        def one(n):
            chip = nth(n)
            rs_pal(b, g, h, chip, c).wait_recv()
            add_into(bucket(b, g, h, chip, c), sibl.at[number(b, g, h), chip])

            @pl.when((z == 0) & (n < last))
            def _():
                rs_hop(0, b, g, h, n + 1, chip).start()

            @pl.when((z == last) & (n < last))
            def _():
                rs_hop(1, b, g, h, n + 1, chip).start()

        steps(0, chips, one)

    def rs_service(b, g, h):
        q = number(b, g, h)

        def one(k):
            @pl.when((z >= 1) & (k >= z))
            def _():
                dest = chips - k + z - 1
                rs_hop(0, b, g, h, k, dest).wait_recv()
                add_into(bucket(b, g, h, dest, c), rland.at[0, q, k - 1])
                rs_hop(0, b, g, h, k + 1, dest).start()

            @pl.when((z < last) & (k >= last - z))
            def _():
                dest = z + k - last
                rs_hop(1, b, g, h, k, dest).wait_recv()
                add_into(bucket(b, g, h, dest, c), rland.at[1, q, k - 1])
                rs_hop(1, b, g, h, k + 1, dest).start()

        steps(1, last, one)

    def rs_finish(b, g, h):
        q = number(b, g, h)

        @pl.when(z >= 1)
        def _():
            rs_hop(0, b, g, h, last, z).wait_recv()

        @pl.when(z < last)
        def _():
            rs_hop(1, b, g, h, last, z).wait_recv()

        own = bucket(b, g, h, z, c)

        def put(*others):
            for at in range(0, sub, strip):
                value = own[:, pl.ds(at, strip)].astype(f32)
                for other in others:
                    value = value + other[:, pl.ds(at, strip)].astype(f32)
                reduced[b, g, :, pl.ds(h * sub + at, strip)] = value.astype(bf)

        @pl.when(z == 0)
        def _():
            put(rland.at[1, q, last - 1])

        @pl.when(z == last)
        def _():
            put(rland.at[0, q, last - 1])

        @pl.when((z > 0) & (z < last))
        def _():
            put(rland.at[0, q, last - 1], rland.at[1, q, last - 1])

    def rs_drain(b, g, h):
        steps(0, chips, lambda chip: rs_pal(b, g, h, chip, 1 - c).wait_send())

        def one(k):
            @pl.when(k >= z + 1)
            def _():
                rs_hop(0, b, g, h, k, chips - k + z).wait_send()

            @pl.when(k >= chips - z)
            def _():
                rs_hop(1, b, g, h, k, k - chips + z).wait_send()

        steps(1, chips, one)

    def sec_hop(b, g, h, k, owner):
        q = number(b, g, h)
        at = pl.ds(h * sub, sub)
        return remote(
            reduced.at[b, g, :, at], every.at[owner, b, g, :, at],
            sec_send.at[q, k - 1], sec_recv.at[q, k - 1],
            {"section": lax.rem(me + k, sections)},
        )

    def own_put(b, g, h):
        at = pl.ds(h * sub, sub)
        return pltpu.make_async_copy(
            reduced.at[b, g, :, at], every.at[me, b, g, :, at], put_sem.at[number(b, g, h)]
        )

    def sec_start(b, g, h):
        for k in range(1, sections):
            sec_hop(b, g, h, k, me).start()
        own_put(b, g, h).start()

    def sec_drain(b, g, h):
        for k in range(1, sections):
            sec_hop(b, g, h, k, lax.rem(me + sections - k, sections)).wait_recv()
        for k in range(1, sections):
            sec_hop(b, g, h, k, me).wait_send()
        own_put(b, g, h).wait()

    def contract(b, g, h):
        out = jnp.zeros((combos, cond_width), f32)
        for p in range(per):
            for at in range(h * sub, (h + 1) * sub, strip):
                out += lax.dot_general(
                    reduced[b, g, p * combos : (p + 1) * combos, pl.ds(at, strip)],
                    gens[g, :, pl.ds(p * piece + at, strip)], nt, preferred_element_type=f32,
                )
        part[b] += out

    def slot_hop(k, owner):
        ref = slots_all.at[owner]
        return remote(
            slots_own, ref, slot_send.at[k - 1], slot_recv.at[k - 1],
            {"section": lax.rem(me + k, sections)},
        )

    def sum_hop(k):
        return remote(
            sums.at[d], sums.at[d], sum_send.at[k - 1], sum_recv.at[d],
            {"dp": lax.rem(d + k, ways)},
        )

    def task_hop(k, owner):
        return remote(
            task_out.at[owner], task_out.at[owner], task_send.at[k - 1], task_recv.at[k - 1],
            {"section": lax.rem(me + k, sections)},
        )

    top = blocks - 1
    pieces = [(g, h) for g in (0, 1) for h in range(parts)]
    generate(0)
    pl.semaphore_wait(barrier, ways - 1 + sections - 1)
    ag_start(top, 0)
    generate(1)
    ag_start(top, 1)
    for k in range(1, sections):
        slot_hop(k, me).start()
    weigh()
    part[...] = jnp.zeros_like(part)
    hid_copy.wait()
    norm(top)

    def both(fn, b, k):
        for g in (0, 1):
            fn(b, g, k)

    steps(1, last, lambda k: both(ag_service, top, k))
    if top > 0:
        for g in (0, 1):
            ag_start(top - 1, g)
    for b in reversed(range(top)):
        norm(b)
    for k in range(1, sections):
        slot_hop(k, lax.rem(me + sections - k, sections)).wait_recv()
    slots_all[me] = slots_own[...]
    pre_all = task[...][None, None, :, None, :] + slots_all[...][:, :, None, :, :]
    cond_all[...] = (
        (pre_all / (1.0 + jnp.exp(-pre_all))).reshape(sections * blocks * combos, cond_width).astype(bf)
    )
    ag_service(top, 0, last)
    ag_finish(top, 0)
    project(top)
    ag_service(top, 1, last)
    ag_finish(top, 1)

    @pl.when(me == sections - 1)
    def _():
        pltpu.make_async_copy(grad_in, landed.at[pl.ds(0, micro)], in_sem.at[1]).wait()

    early = me < sections // 2
    for b in reversed(range(blocks)):
        ready, later = [], pieces
        if b < top:
            ready, later = pieces[:parts], pieces[parts:]

            @pl.when(early)
            def _():
                for g, h in ready:
                    rs_service(b + 1, g, h)

        if b > 0 and last > 1:
            @pl.when(early)
            def _():
                both(ag_service, b - 1, 1)

        def between(m):
            if b > 0 and last > 1:
                @pl.when(jnp.logical_not(early) & (m == micro // 2))
                def _():
                    ag_service(b - 1, 0, 1)

            if b < top:
                @pl.when(early & (m == micro // 2))
                def _():
                    rs_service(b + 1, *later[0])

        relay(b, between)
        if b > 0:
            if last > 1:
                @pl.when(jnp.logical_not(early))
                def _():
                    ag_service(b - 1, 1, 1)

        if b < top:
            @pl.when(jnp.logical_not(early))
            def _():
                for g, h in ready + later[:1]:
                    rs_service(b + 1, g, h)

            for g, h in later[1:]:
                rs_service(b + 1, g, h)
        for g in (0, 1):
            grads(b, g)
            if b == 0:
                rs_exchange(b, g)
        if b > 0:
            steps(2, last, lambda k: both(ag_service, b - 1, k))
            for g in (0, 1):
                rs_exchange(b, g)
            for g, h in pieces:
                rs_start(b, g, h)
            ag_service(b - 1, 0, last)
            ag_finish(b - 1, 0)
            project(b - 1)
            ag_service(b - 1, 1, last)
            ag_finish(b - 1, 1)
            if b - 1 > 0:
                for g in (0, 1):
                    ag_start(b - 2, g)
        else:
            for g, h in pieces:
                rs_start(b, g, h)
        if b < top:
            for g, h in pieces:
                rs_finish(b + 1, g, h)
                sec_start(b + 1, g, h)
            for g, h in pieces:
                contract(b + 1, g, h)
    for g, h in pieces:
        rs_service(0, g, h)
        rs_finish(0, g, h)
        sec_start(0, g, h)
        contract(0, g, h)

    d_pre = part[...].reshape(blocks, tasks, experts, cond_width) * sig * (1.0 + pre * (1.0 - sig))
    slot_rows = blocks * experts
    sums[d] = jnp.zeros_like(sums[d])
    sums[d, pl.ds(0, slot_rows)] = jnp.sum(d_pre, axis=1).reshape(slot_rows, cond_width)
    sums[d, pl.ds(slot_rows, tasks)] = jnp.sum(d_pre, axis=(0, 2))
    steps(1, ways, lambda k: sum_hop(k).start())

    def sum_wait(k):
        other = lax.rem(d + k, ways)
        remote(
            sums.at[other], sums.at[other], sum_send.at[k - 1], sum_recv.at[other], {"dp": other}
        ).wait_recv()

    steps(1, ways, sum_wait)
    whole = jnp.sum(sums[...], axis=0)
    slot_out[...] = whole[:slot_rows]
    task_out[me] = whole[slot_rows:]
    for k in range(1, sections):
        task_hop(k, me).start()

    for b in range(blocks):
        for g in (0, 1):
            ag_drain(b, g)
        for g, h in pieces:
            rs_drain(b, g, h)
    steps(0, total, relay_drain)
    steps(0, micro, lambda m: hid_put(m).wait())
    steps(1, ways, lambda k: sum_hop(k).wait_send())
    for k in range(1, sections):
        slot_hop(k, me).wait_send()
        task_hop(k, lax.rem(me + sections - k, sections)).wait_recv()
        task_hop(k, me).wait_send()
    for b in range(blocks):
        for g, h in pieces:
            sec_drain(b, g, h)


def generators(
    cond, every, hid, slot_sum, task_sums, hid_out, down, up, task_out, slot_out
):
    rows = cond.shape[0]
    for g, out in ((0, down), (1, up)):
        right = every[:, :, g].reshape(rows, every.shape[-1])
        out[...] = lax.dot_general(cond[...], right, tn, preferred_element_type=f32)
    hid_out[...] = hid[...]
    slot_out[...] = slot_sum[...]
    task_out[...] = jnp.sum(task_sums[...], axis=0)[: task_out.shape[0]]


def on_device(
    hidden_in, out_grad, gate_probs, expert_ids, task_ids, task_embed, slot_embed, gen_down, gen_up
):
    sections, ways = lax.axis_size("section"), lax.axis_size("dp")
    blocks, _, micro, tok, width = hidden_in.shape
    tasks, cond_width = task_embed.shape
    experts = slot_embed.shape[2]
    combos = tasks * experts
    span = gen_down.shape[1]
    per = max(1, span // width)
    cuts = max(1, width // span)
    piece = span // per
    rows = per * combos
    groups = ways // cuts
    ranks = groups * rows
    total, tokens, chips = blocks * micro, micro * tok, ways // 2
    quads = 2 * blocks
    chunk = min(piece, 1024)

    slots_own = slot_embed[:, 0]
    gates = gate_probs[:, 0].transpose(0, 1, 3, 2)
    picks = expert_ids[:, 0].transpose(0, 1, 3, 2)
    parts = 2
    sub = piece // parts

    vmem = pl.BlockSpec(memory_space=pltpu.VMEM)
    anywhere = pl.BlockSpec(memory_space=pl.ANY)
    sem = pltpu.SemaphoreType.DMA
    sizes = (sections, ways, blocks, micro, tok, width, tasks, experts, per, cuts, piece)
    hidden, every, cond_all, slot_sum, task_sums = pl.pallas_call(
        functools.partial(backward, sizes),
        out_shape=(
            jax.ShapeDtypeStruct((micro, tok, width), bf),
            jax.ShapeDtypeStruct((sections, blocks, 2, rows, piece), bf),
            jax.ShapeDtypeStruct((sections * blocks * combos, cond_width), bf),
            jax.ShapeDtypeStruct((blocks * experts, cond_width), f32),
            jax.ShapeDtypeStruct((sections, 8, cond_width), f32),
        ),
        in_specs=[
            anywhere, anywhere, vmem, vmem, pl.BlockSpec(memory_space=pltpu.SMEM), vmem, vmem,
            anywhere, anywhere,
        ],
        out_specs=(anywhere, anywhere, vmem, vmem, vmem),
        scratch_shapes=[
            pltpu.VMEM((2, cond_width, span), bf),
            pltpu.VMEM((blocks, tokens, width), bf),
            pltpu.VMEM((blocks, tokens, width), bf),
            pltpu.VMEM((blocks, tokens, 1), f32),
            pltpu.VMEM((blocks, tokens, ranks), f32),
            pltpu.VMEM((blocks, tokens, ranks), bf),
            pltpu.VMEM((blocks, tokens, ranks), bf),
            pltpu.VMEM((total, tok, width), bf),
            pltpu.VMEM((total, tok, width), bf),
            pltpu.VMEM((blocks, 2, cuts, groups, rows, piece), bf),
            pltpu.VMEM((blocks, 2, cuts, groups, rows, piece), bf),
            pltpu.VMEM((quads * parts, chips, rows, sub), bf),
            pltpu.VMEM((2, quads * parts, chips - 1, rows, sub), bf),
            pltpu.VMEM((blocks, tokens, ranks), f32),
            pltpu.VMEM((blocks, 2, rows, piece), bf),
            pltpu.VMEM((sections, blocks, experts, cond_width), f32),
            pltpu.VMEM((blocks, combos, cond_width), f32),
            pltpu.VMEM((ways, blocks * experts + 8, cond_width), f32),
            sem((2, span // chunk)),
            sem((2,)),
            sem((micro,)),
            sem((quads * parts,)),
            sem((2, quads, chips - 1)),
            sem((2, quads, chips - 1)),
            sem((quads, chips)),
            sem((quads, chips)),
            sem((quads * parts, chips)),
            sem((quads * parts, chips)),
            sem((2, quads * parts, chips - 1)),
            sem((2, quads * parts, chips - 1)),
            sem((quads * parts, sections - 1)),
            sem((quads * parts, sections - 1)),
            sem((total, 4)),
            sem((total, 4)),
            sem((sections - 1,)),
            sem((sections - 1,)),
            sem((ways - 1,)),
            sem((ways,)),
            sem((sections - 1,)),
            sem((sections - 1,)),
        ],
        compiler_params=pltpu.CompilerParams(
            collective_id=1, has_side_effects=True, vmem_limit_bytes=58 << 20
        ),
        name="backward",
    )(
        hidden_in.reshape(blocks, tokens, width), out_grad, gates, picks, task_ids, slots_own,
        task_embed, gen_down, gen_up,
    )

    out_chunk = min(piece, 1024)
    across = piece // out_chunk
    strip = width // (per * across)
    here = pl.BlockSpec((tokens, strip), lambda p, i: (0, p * across + i))
    columns = pl.BlockSpec((cond_width, out_chunk), lambda p, i: (0, p * across + i))

    def fixed(*shape):
        return pl.BlockSpec(shape, lambda p, i: (0,) * len(shape))

    d_hidden, d_down, d_up, d_task, d_slot = pl.pallas_call(
        generators,
        grid=(per, across),
        out_shape=(
            jax.ShapeDtypeStruct((tokens, width), bf),
            jax.ShapeDtypeStruct((cond_width, span), f32),
            jax.ShapeDtypeStruct((cond_width, span), f32),
            jax.ShapeDtypeStruct((tasks, cond_width), f32),
            jax.ShapeDtypeStruct((blocks * experts, cond_width), f32),
        ),
        in_specs=[
            fixed(sections * blocks * combos, cond_width),
            pl.BlockSpec((sections, blocks, 2, combos, out_chunk), lambda p, i: (0, 0, 0, p, i)),
            here,
            fixed(blocks * experts, cond_width),
            fixed(sections, 8, cond_width),
        ],
        out_specs=(
            here, columns, columns, fixed(tasks, cond_width), fixed(blocks * experts, cond_width)
        ),
        compiler_params=pltpu.CompilerParams(vmem_limit_bytes=58 << 20),
        name="generators",
    )(cond_all, every, hidden.reshape(tokens, width), slot_sum, task_sums)
    return (
        d_hidden.reshape(1, micro, tok, width), d_down, d_up, d_task,
        d_slot.reshape(blocks, 1, experts, cond_width),
    )


def solution(mesh):
    placed = (
        P(None, "section", None, "dp", None),
        P(None, "dp", None),
        P(None, "section", None, "dp", None),
        P(None, "section", None, "dp", None),
        P(None, "dp"),
        P(),
        P(None, "section", None, None),
        P(None, "dp"),
        P(None, "dp"),
    )
    return jax.shard_map(
        on_device,
        mesh=mesh,
        in_specs=placed,
        out_specs=(
            P("section", None, "dp", None),
            P(None, "dp"),
            P(None, "dp"),
            P(),
            P(None, "section", None, None),
        ),
        check_vma=False,
    )
```

```python
import functools

import jax
import jax.numpy as jnp
from jax import lax
from jax.experimental import pallas as pl
from jax.experimental.pallas import tpu as pltpu
from jax.sharding import PartitionSpec as P

eps = 1e-05
MESH = pl.DeviceIdType.MESH
nt = (((1,), (1,)), ((), ()))
tn = (((0,), (0,)), ((), ()))
f32 = jnp.float32
bf = jnp.bfloat16


def backward(
    sizes,
    hid_in, grad_in, gates, picks, task_ids, slots_own, task, gen_down, gen_up,
    hid_out, every, cond_all, slot_out, task_out,
    gens, hid, xn, inv_s, low_s, low_w, glow_s, landed, made, adapt, gpart, sibl, rland,
    cols, reduced, slots_all, part, sums,
    gen_sem, in_sem, out_sem, put_sem, ag_send, ag_recv, sib_send, sib_recv, rsib_send, rsib_recv, rs_send, rs_recv,
    sec_send, sec_recv, rel_send, rel_recv, slot_send, slot_recv, sum_send, sum_recv,
    task_send, task_recv,
):
    sections, ways, blocks, micro, tok, width, tasks, experts, per, cuts, piece = sizes
    me, d = lax.axis_index("section"), lax.axis_index("dp")
    chips = ways // 2
    z, c = d // 2, lax.rem(d, 2)
    pal = d + 1 - 2 * c
    last = chips - 1
    combos = tasks * experts
    rows = per * combos
    groups = ways // cuts
    ranks = groups * rows
    cond_width = gens.shape[1]
    chunk = min(piece, 1024)
    hop = width // 4
    parts = rland.shape[1] // (2 * blocks)
    sub = rows // parts
    tokens = micro * tok
    total = blocks * micro
    below, above = lax.rem(me + sections - 1, sections), lax.rem(me + 1, sections)
    scale = 1.0 / (micro * tok * ways)

    def remote(src, dst, send, recv, where):
        return pltpu.make_async_remote_copy(
            src_ref=src, dst_ref=dst, send_sem=send, recv_sem=recv,
            device_id=where, device_id_type=MESH,
        )

    def steps(low, high, body):
        def run(k, carry):
            body(k)
            return carry

        lax.fori_loop(low, high, run, 0)

    gen_copies = []
    for g, source in ((0, gen_down), (1, gen_up)):
        for n, at in enumerate(range(0, per * piece, chunk)):
            gen_copies.append(
                pltpu.make_async_copy(
                    source.at[:, pl.ds(at, chunk)], gens.at[g, :, pl.ds(at, chunk)], gen_sem.at[g, n]
                )
            )
            gen_copies[-1].start()
    hid_copy = pltpu.make_async_copy(hid_in, hid, in_sem.at[0])
    hid_copy.start()

    @pl.when(me == sections - 1)
    def _():
        pltpu.make_async_copy(grad_in, landed.at[pl.ds(0, micro)], in_sem.at[1]).start()

    barrier = pltpu.get_barrier_semaphore()

    def greet_dp(k):
        pl.semaphore_signal(
            barrier, inc=1, device_id={"dp": lax.rem(d + k, ways)}, device_id_type=MESH
        )

    def greet_section(k):
        pl.semaphore_signal(
            barrier, inc=1, device_id={"section": lax.rem(me + k, sections)}, device_id_type=MESH
        )

    steps(1, ways, greet_dp)
    steps(1, sections, greet_section)

    my_cut, my_group = lax.rem(d, cuts), d // cuts
    pre = task[...][None, :, None, :] + slots_own[...][:, None, :, :]
    sig = 1.0 / (1.0 + jnp.exp(-pre))
    cond = (pre * sig).reshape(blocks * combos, cond_width).astype(bf)

    def weigh():
        eye = lax.broadcasted_iota(jnp.int32, (tok, tok), 0) == lax.broadcasted_iota(
            jnp.int32, (tok, tok), 1
        )
        lane = lax.broadcasted_iota(jnp.int32, (tok, ranks), 1)
        expert = lax.rem(lane, experts).astype(f32)
        task_of = lax.rem(lane, combos) // experts

        def column(row):
            return jnp.sum(jnp.where(eye, row, 0.0), axis=1, keepdims=True)

        for m in range(micro):
            right_task = jnp.where(task_of == task_ids[m], 1.0, 0.0)
            for b in range(blocks):
                total_weight = jnp.zeros((tok, ranks), f32)
                for k in range(gates.shape[2]):
                    pick = column(picks[b, m, k : k + 1].astype(f32))
                    gate = column(gates[b, m, k : k + 1])
                    total_weight += jnp.where(pick == expert, gate, 0.0)
                cols[b, m * tok : (m + 1) * tok] = right_task * total_weight

    def generate(g):
        for n, at in enumerate(range(0, per * piece, chunk)):
            gen_copies[g * (per * piece // chunk) + n].wait()
            out = jnp.dot(cond, gens[g, :, pl.ds(at, chunk)], preferred_element_type=f32).astype(bf)
            row, col = at // piece * combos, at % piece
            for b in range(blocks):
                adapt[b, g, my_cut, my_group, pl.ds(row, combos), pl.ds(col, chunk)] = out[
                    b * combos : (b + 1) * combos
                ]

    def shard(b, g, chip, core):
        dev = 2 * chip + core
        return adapt.at[b, g, lax.rem(dev, cuts), dev // cuts]

    def ag_hop(side, b, g, k, chip):
        ref = shard(b, g, chip, c)
        q = 2 * b + g
        to = d + 2 if side == 0 else d - 2
        return remote(
            ref, ref, ag_send.at[side, q, k - 1], ag_recv.at[side, q, k - 1], {"dp": to}
        )

    def ag_pal(b, g, chip, core):
        ref = shard(b, g, chip, core)
        q = 2 * b + g
        return remote(ref, ref, sib_send.at[q, chip], sib_recv.at[q, chip], {"dp": pal})

    def ag_start(b, g):
        @pl.when(z < last)
        def _():
            ag_hop(0, b, g, 1, z).start()

        @pl.when(z > 0)
        def _():
            ag_hop(1, b, g, 1, z).start()

        ag_pal(b, g, z, c).start()

    def ag_service(b, g, k):
        @pl.when(z >= k)
        def _():
            ag_hop(0, b, g, k, z - k).wait_recv()

            @pl.when((z < last) & (k < last))
            def _():
                ag_hop(0, b, g, k + 1, z - k).start()

            ag_pal(b, g, z - k, c).start()

        @pl.when(z + k <= last)
        def _():
            ag_hop(1, b, g, k, z + k).wait_recv()

            @pl.when((z > 0) & (k < last))
            def _():
                ag_hop(1, b, g, k + 1, z + k).start()

            ag_pal(b, g, z + k, c).start()

    def ag_finish(b, g):
        steps(0, chips, lambda chip: ag_pal(b, g, chip, 1 - c).wait_recv())

    def ag_drain(b, g):
        def one(k):
            @pl.when((z < last) & (z - k + 1 >= 0))
            def _():
                ag_hop(0, b, g, k, z - k + 1).wait_send()

            @pl.when((z > 0) & (z + k - 1 <= last))
            def _():
                ag_hop(1, b, g, k, z + k - 1).wait_send()

        steps(1, chips, one)
        steps(0, chips, lambda chip: ag_pal(b, g, chip, c).wait_send())

    def spans(size):
        for at in range(0, width, size):
            yield at, at // piece, at % piece

    def panel(b, g, at, size):
        return adapt[b, g, at // piece, :, :, pl.ds(at % piece, size)].reshape(ranks, size)

    def norm(b):
        square = jnp.zeros((tokens, 1), f32)
        for at, _, _ in spans(chunk):
            x = hid[b, :, pl.ds(at, chunk)].astype(f32)
            square += jnp.sum(x * x, axis=-1, keepdims=True)
        inv = lax.rsqrt(square * (1.0 / width) + eps)
        inv_s[b] = inv
        for at, _, _ in spans(chunk):
            xn[b, :, pl.ds(at, chunk)] = (hid[b, :, pl.ds(at, chunk)].astype(f32) * inv).astype(bf)

    def project(b):
        low = jnp.zeros((tokens, ranks), f32)
        for at, _, _ in spans(chunk):
            low += lax.dot_general(
                xn[b, :, pl.ds(at, chunk)], panel(b, 0, at, chunk), nt, preferred_element_type=f32
            )
        low_s[b] = low
        low_w[b] = (cols[b] * low).astype(bf)

    def relay_hop(item, slot, n):
        at = pl.ds(n * hop, hop)
        return remote(
            made.at[item, :, at], landed.at[slot, :, at],
            rel_send.at[item, n], rel_recv.at[slot, n], {"section": below},
        )

    def hid_put(m):
        return pltpu.make_async_copy(
            made.at[total - micro + m], hid_out.at[m], out_sem.at[m]
        )

    def relay(b, between):
        first_item = (blocks - 1 - b) * micro

        def one(m):
            item = first_item + m
            between(m)
            mine = pl.ds(pl.multiple_of(m * tok, tok), tok)
            back = jnp.zeros((tok, ranks), f32)
            for n in range(4):
                if b == blocks - 1:
                    @pl.when(me < sections - 1)
                    def _():
                        relay_hop(item, item, n).wait_recv()
                else:
                    relay_hop(item, item, n).wait_recv()
                for at in range(n * hop, (n + 1) * hop, min(hop, chunk)):
                    back += lax.dot_general(
                        landed[item, :, pl.ds(at, min(hop, chunk))], panel(b, 1, at, min(hop, chunk)),
                        nt, preferred_element_type=f32,
                    )
            glow = (cols[b, mine] * back).astype(bf)
            glow_s[b, mine] = glow
            dots = jnp.sum(glow.astype(f32) * low_s[b, mine], axis=-1, keepdims=True) * (1.0 / width)
            inv = inv_s[b, mine]
            scaled = dots * inv
            for n in range(4):
                for at in range(n * hop, (n + 1) * hop, min(hop, chunk)):
                    size = min(hop, chunk)
                    up = jnp.dot(glow, panel(b, 0, at, size), preferred_element_type=f32)
                    xf = hid[b, mine, pl.ds(at, size)].astype(f32) * inv
                    dx = landed[item, :, pl.ds(at, size)].astype(f32) + (inv * up - xf * scaled)
                    dx = dx.astype(bf)
                    made[item, :, pl.ds(at, size)] = dx

                @pl.when(me > 0)
                def _():
                    relay_hop(item, item, n).start()

                if b > 0:
                    @pl.when(me == 0)
                    def _():
                        relay_hop(item, item + micro, n).start()

            if b == 0:
                hid_put(m).start()

        steps(0, micro, one)

    def relay_drain(item):
        for n in range(4):
            @pl.when((me > 0) | (item < total - micro))
            def _():
                relay_hop(item, item, n).wait_send()

    def grads(b, g):
        base = (blocks - 1 - b) * micro
        left = (glow_s if g == 0 else low_w)[b]
        for at, cut, col in spans(chunk):
            if g == 0:
                right = xn[b, :, pl.ds(at, chunk)]
            else:
                right = landed[pl.ds(base, micro), :, pl.ds(at, chunk)].reshape(tokens, chunk)
            out = lax.dot_general(left, right, tn, preferred_element_type=f32) * scale
            gpart[b, g, cut, :, :, pl.ds(col, chunk)] = out.astype(bf).reshape(groups, rows, chunk)

    def bucket(b, g, h, chip, core):
        dev = 2 * chip + core
        return gpart.at[b, g, lax.rem(dev, cuts), dev // cuts, pl.ds(h * sub, sub)]

    def number(b, g, h):
        return (2 * b + g) * parts + h

    def rs_pal(b, g, h, chip, core):
        q = number(b, g, h)
        return remote(
            bucket(b, g, h, chip, core), sibl.at[q, chip],
            rsib_send.at[q, chip], rsib_recv.at[q, chip], {"dp": pal},
        )

    def rs_hop(side, b, g, h, k, dest):
        q = number(b, g, h)
        to = d + 2 if side == 0 else d - 2
        return remote(
            bucket(b, g, h, dest, c), rland.at[side, q, k - 1],
            rs_send.at[side, q, k - 1], rs_recv.at[side, q, k - 1], {"dp": to},
        )

    def add_into(target, *others):
        for at in range(0, piece, chunk):
            value = target[:, pl.ds(at, chunk)].astype(f32)
            for other in others:
                value = value + other[:, pl.ds(at, chunk)].astype(f32)
            target[:, pl.ds(at, chunk)] = value.astype(bf)

    def nth(n):
        return jnp.where(2 * z < chips, last - n, n)

    def rs_exchange(b, g):
        for h in range(parts):
            steps(0, chips, lambda n: rs_pal(b, g, h, nth(n), 1 - c).start())

    def rs_start(b, g, h):
        def one(n):
            chip = nth(n)
            rs_pal(b, g, h, chip, c).wait_recv()
            add_into(bucket(b, g, h, chip, c), sibl.at[number(b, g, h), chip])

            @pl.when((z == 0) & (n < last))
            def _():
                rs_hop(0, b, g, h, n + 1, chip).start()

            @pl.when((z == last) & (n < last))
            def _():
                rs_hop(1, b, g, h, n + 1, chip).start()

        steps(0, chips, one)

    def rs_service(b, buckets, low, high):
        def one(k):
            for g, h in buckets:
                rs_step(b, g, h, k)

        if high > low:
            steps(low, high, one)

    def rs_step(b, g, h, k):
        q = number(b, g, h)

        @pl.when((z >= 1) & (k >= z))
        def _():
            dest = chips - k + z - 1
            rs_hop(0, b, g, h, k, dest).wait_recv()
            add_into(bucket(b, g, h, dest, c), rland.at[0, q, k - 1])
            rs_hop(0, b, g, h, k + 1, dest).start()

        @pl.when((z < last) & (k >= last - z))
        def _():
            dest = z + k - last
            rs_hop(1, b, g, h, k, dest).wait_recv()
            add_into(bucket(b, g, h, dest, c), rland.at[1, q, k - 1])
            rs_hop(1, b, g, h, k + 1, dest).start()

    def rs_finish(b, g, h):
        q = number(b, g, h)

        @pl.when(z >= 1)
        def _():
            rs_hop(0, b, g, h, last, z).wait_recv()

        @pl.when(z < last)
        def _():
            rs_hop(1, b, g, h, last, z).wait_recv()

        own = bucket(b, g, h, z, c)

        def put(*others):
            for at in range(0, piece, chunk):
                value = own[:, pl.ds(at, chunk)].astype(f32)
                for other in others:
                    value = value + other[:, pl.ds(at, chunk)].astype(f32)
                reduced[b, g, pl.ds(h * sub, sub), pl.ds(at, chunk)] = value.astype(bf)

        @pl.when(z == 0)
        def _():
            put(rland.at[1, q, last - 1])

        @pl.when(z == last)
        def _():
            put(rland.at[0, q, last - 1])

        @pl.when((z > 0) & (z < last))
        def _():
            put(rland.at[0, q, last - 1], rland.at[1, q, last - 1])

    def rs_drain(b, g, h):
        steps(0, chips, lambda chip: rs_pal(b, g, h, chip, 1 - c).wait_send())

        def one(k):
            @pl.when(k >= z + 1)
            def _():
                rs_hop(0, b, g, h, k, chips - k + z).wait_send()

            @pl.when(k >= chips - z)
            def _():
                rs_hop(1, b, g, h, k, k - chips + z).wait_send()

        steps(1, chips, one)

    def sec_hop(b, g, h, k, owner):
        q = number(b, g, h)
        at = pl.ds(h * sub, sub)
        return remote(
            reduced.at[b, g, at], every.at[owner, b, g, at],
            sec_send.at[q, k - 1], sec_recv.at[q, k - 1],
            {"section": lax.rem(me + k, sections)},
        )

    def own_put(b, g, h):
        at = pl.ds(h * sub, sub)
        return pltpu.make_async_copy(
            reduced.at[b, g, at], every.at[me, b, g, at], put_sem.at[number(b, g, h)]
        )

    def sec_start(b, g, h):
        for k in range(1, sections):
            sec_hop(b, g, h, k, me).start()
        own_put(b, g, h).start()

    def sec_drain(b, g, h):
        for k in range(1, sections):
            sec_hop(b, g, h, k, lax.rem(me + sections - k, sections)).wait_recv()
        for k in range(1, sections):
            sec_hop(b, g, h, k, me).wait_send()
        own_put(b, g, h).wait()

    def contract(b, g, h):
        out = jnp.zeros((combos, cond_width), f32)
        for row in range(h * sub, (h + 1) * sub, combos):
            for at in range(0, piece, chunk):
                out += lax.dot_general(
                    reduced[b, g, row : row + combos, pl.ds(at, chunk)],
                    gens[g, :, pl.ds(row // combos * piece + at, chunk)], nt,
                    preferred_element_type=f32,
                )
        part[b] += out

    def slot_hop(k, owner):
        ref = slots_all.at[owner]
        return remote(
            slots_own, ref, slot_send.at[k - 1], slot_recv.at[k - 1],
            {"section": lax.rem(me + k, sections)},
        )

    def sum_hop(k):
        return remote(
            sums.at[d], sums.at[d], sum_send.at[k - 1], sum_recv.at[d],
            {"dp": lax.rem(d + k, ways)},
        )

    def task_hop(k, owner):
        return remote(
            task_out.at[owner], task_out.at[owner], task_send.at[k - 1], task_recv.at[k - 1],
            {"section": lax.rem(me + k, sections)},
        )

    top = blocks - 1
    pieces = [(g, h) for g in (0, 1) for h in range(parts)]
    generate(0)
    pl.semaphore_wait(barrier, ways - 1 + sections - 1)
    ag_start(top, 0)
    generate(1)
    ag_start(top, 1)
    for k in range(1, sections):
        slot_hop(k, me).start()
    weigh()
    part[...] = jnp.zeros_like(part)
    hid_copy.wait()
    norm(top)

    def both(fn, b, k):
        for g in (0, 1):
            fn(b, g, k)

    steps(1, last, lambda k: both(ag_service, top, k))
    if top > 0:
        for g in (0, 1):
            ag_start(top - 1, g)
    for b in reversed(range(top)):
        norm(b)
    for k in range(1, sections):
        slot_hop(k, lax.rem(me + sections - k, sections)).wait_recv()
    slots_all[me] = slots_own[...]
    pre_all = task[...][None, None, :, None, :] + slots_all[...][:, :, None, :, :]
    cond_all[...] = (
        (pre_all / (1.0 + jnp.exp(-pre_all))).reshape(sections * blocks * combos, cond_width).astype(bf)
    )
    ag_service(top, 0, last)
    ag_finish(top, 0)
    project(top)
    ag_service(top, 1, last)
    ag_finish(top, 1)

    @pl.when(me == sections - 1)
    def _():
        pltpu.make_async_copy(grad_in, landed.at[pl.ds(0, micro)], in_sem.at[1]).wait()

    early = me < sections // 2
    late = jnp.logical_not(early)
    first, rest = pieces[:parts], pieces[parts:]
    turn, half = min(2, last), (parts + 1) // 2
    for b in reversed(range(blocks)):
        if b < top:
            @pl.when(early)
            def _():
                rs_service(b + 1, first, 1, last)

        if b > 0 and last > 1:
            @pl.when(early)
            def _():
                both(ag_service, b - 1, 1)

        def between(m):
            if b > 0 and last > 1:
                @pl.when(late & (m == micro // 2))
                def _():
                    ag_service(b - 1, 0, 1)

            if b < top:
                @pl.when(early & (m == micro // 4))
                def _():
                    rs_service(b + 1, rest[:half], 1, turn)

                @pl.when(early & (m == micro - 1))
                def _():
                    rs_service(b + 1, rest[:half], turn, last)
                    rs_service(b + 1, rest[half:], 1, turn)

        relay(b, between)
        if b > 0:
            if last > 1:
                @pl.when(late)
                def _():
                    ag_service(b - 1, 1, 1)

            for g in (0, 1):
                grads(b, g)
                rs_exchange(b, g)
                steps(2, last, lambda k: ag_service(b - 1, g, k))
            for g, h in pieces:
                rs_start(b, g, h)
            ag_service(b - 1, 0, last)
            ag_finish(b - 1, 0)
            project(b - 1)
            ag_service(b - 1, 1, last)
            ag_finish(b - 1, 1)
            if b - 1 > 0:
                for g in (0, 1):
                    ag_start(b - 2, g)
        if b < top:
            @pl.when(late)
            def _():
                rs_service(b + 1, pieces, 1, turn)

        if b == 0:
            for g in (0, 1):
                grads(b, g)
                rs_exchange(b, g)
            for g, h in pieces:
                rs_start(b, g, h)
        if b < top:
            @pl.when(late)
            def _():
                rs_service(b + 1, pieces, turn, last)

            @pl.when(early)
            def _():
                rs_service(b + 1, rest[half:], turn, last)

            for g, h in pieces:
                rs_finish(b + 1, g, h)
                sec_start(b + 1, g, h)
    for n in range(len(pieces) + 1):
        if n < len(pieces):
            rs_service(0, pieces[n : n + 1], 1, last)
        if n > 0:
            g, h = pieces[n - 1]
            rs_finish(0, g, h)
            sec_start(0, g, h)
            for b in range(blocks):
                contract(b, g, h)

    d_pre = part[...].reshape(blocks, tasks, experts, cond_width) * sig * (1.0 + pre * (1.0 - sig))
    slot_rows = blocks * experts
    sums[d] = jnp.zeros_like(sums[d])
    sums[d, pl.ds(0, slot_rows)] = jnp.sum(d_pre, axis=1).reshape(slot_rows, cond_width)
    sums[d, pl.ds(slot_rows, tasks)] = jnp.sum(d_pre, axis=(0, 2))
    steps(1, ways, lambda k: sum_hop(k).start())

    def sum_wait(k):
        other = lax.rem(d + k, ways)
        remote(
            sums.at[other], sums.at[other], sum_send.at[k - 1], sum_recv.at[other], {"dp": other}
        ).wait_recv()

    steps(1, ways, sum_wait)
    whole = jnp.sum(sums[...], axis=0)
    slot_out[...] = whole[:slot_rows]
    task_out[me] = whole[slot_rows:]
    for k in range(1, sections):
        task_hop(k, me).start()

    for b in range(blocks):
        for g in (0, 1):
            ag_drain(b, g)
        for g, h in pieces:
            rs_drain(b, g, h)
    steps(0, total, relay_drain)
    steps(0, micro, lambda m: hid_put(m).wait())
    steps(1, ways, lambda k: sum_hop(k).wait_send())
    for k in range(1, sections):
        slot_hop(k, me).wait_send()
        task_hop(k, lax.rem(me + sections - k, sections)).wait_recv()
        task_hop(k, me).wait_send()
    for b in range(blocks):
        for g, h in pieces:
            sec_drain(b, g, h)


def generators(
    cond, every, hid, slot_sum, task_sums, hid_out, down, up, task_out, slot_out
):
    rows = cond.shape[0]
    for g, out in ((0, down), (1, up)):
        right = every[:, :, g].reshape(rows, every.shape[-1])
        out[...] = lax.dot_general(cond[...], right, tn, preferred_element_type=f32)
    hid_out[...] = hid[...]
    slot_out[...] = slot_sum[...]
    task_out[...] = jnp.sum(task_sums[...], axis=0)[: task_out.shape[0]]


def on_device(
    hidden_in, out_grad, gate_probs, expert_ids, task_ids, task_embed, slot_embed, gen_down, gen_up
):
    sections, ways = lax.axis_size("section"), lax.axis_size("dp")
    blocks, _, micro, tok, width = hidden_in.shape
    tasks, cond_width = task_embed.shape
    experts = slot_embed.shape[2]
    combos = tasks * experts
    span = gen_down.shape[1]
    per = max(1, span // width)
    cuts = max(1, width // span)
    piece = span // per
    rows = per * combos
    groups = ways // cuts
    ranks = groups * rows
    total, tokens, chips = blocks * micro, micro * tok, ways // 2
    quads = 2 * blocks
    chunk = min(piece, 1024)

    slots_own = slot_embed[:, 0]
    gates = gate_probs[:, 0].transpose(0, 1, 3, 2)
    picks = expert_ids[:, 0].transpose(0, 1, 3, 2)
    parts = per
    sub = rows // parts

    vmem = pl.BlockSpec(memory_space=pltpu.VMEM)
    anywhere = pl.BlockSpec(memory_space=pl.ANY)
    sem = pltpu.SemaphoreType.DMA
    sizes = (sections, ways, blocks, micro, tok, width, tasks, experts, per, cuts, piece)
    hidden, every, cond_all, slot_sum, task_sums = pl.pallas_call(
        functools.partial(backward, sizes),
        out_shape=(
            jax.ShapeDtypeStruct((micro, tok, width), bf),
            jax.ShapeDtypeStruct((sections, blocks, 2, rows, piece), bf),
            jax.ShapeDtypeStruct((sections * blocks * combos, cond_width), bf),
            jax.ShapeDtypeStruct((blocks * experts, cond_width), f32),
            jax.ShapeDtypeStruct((sections, 8, cond_width), f32),
        ),
        in_specs=[
            anywhere, anywhere, vmem, vmem, pl.BlockSpec(memory_space=pltpu.SMEM), vmem, vmem,
            anywhere, anywhere,
        ],
        out_specs=(anywhere, anywhere, vmem, vmem, vmem),
        scratch_shapes=[
            pltpu.VMEM((2, cond_width, span), bf),
            pltpu.VMEM((blocks, tokens, width), bf),
            pltpu.VMEM((blocks, tokens, width), bf),
            pltpu.VMEM((blocks, tokens, 1), f32),
            pltpu.VMEM((blocks, tokens, ranks), f32),
            pltpu.VMEM((blocks, tokens, ranks), bf),
            pltpu.VMEM((blocks, tokens, ranks), bf),
            pltpu.VMEM((total, tok, width), bf),
            pltpu.VMEM((total, tok, width), bf),
            pltpu.VMEM((blocks, 2, cuts, groups, rows, piece), bf),
            pltpu.VMEM((blocks, 2, cuts, groups, rows, piece), bf),
            pltpu.VMEM((quads * parts, chips, sub, piece), bf),
            pltpu.VMEM((2, quads * parts, chips - 1, sub, piece), bf),
            pltpu.VMEM((blocks, tokens, ranks), f32),
            pltpu.VMEM((blocks, 2, rows, piece), bf),
            pltpu.VMEM((sections, blocks, experts, cond_width), f32),
            pltpu.VMEM((blocks, combos, cond_width), f32),
            pltpu.VMEM((ways, blocks * experts + 8, cond_width), f32),
            sem((2, span // chunk)),
            sem((2,)),
            sem((micro,)),
            sem((quads * parts,)),
            sem((2, quads, chips - 1)),
            sem((2, quads, chips - 1)),
            sem((quads, chips)),
            sem((quads, chips)),
            sem((quads * parts, chips)),
            sem((quads * parts, chips)),
            sem((2, quads * parts, chips - 1)),
            sem((2, quads * parts, chips - 1)),
            sem((quads * parts, sections - 1)),
            sem((quads * parts, sections - 1)),
            sem((total, 4)),
            sem((total, 4)),
            sem((sections - 1,)),
            sem((sections - 1,)),
            sem((ways - 1,)),
            sem((ways,)),
            sem((sections - 1,)),
            sem((sections - 1,)),
        ],
        compiler_params=pltpu.CompilerParams(
            collective_id=1, has_side_effects=True, vmem_limit_bytes=58 << 20
        ),
        name="backward",
    )(
        hidden_in.reshape(blocks, tokens, width), out_grad, gates, picks, task_ids.reshape(-1), slots_own,
        task_embed, gen_down, gen_up,
    )

    out_chunk = min(piece, 1024)
    across = piece // out_chunk
    strip = width // (per * across)
    here = pl.BlockSpec((tokens, strip), lambda p, i: (0, p * across + i))
    columns = pl.BlockSpec((cond_width, out_chunk), lambda p, i: (0, p * across + i))

    def fixed(*shape):
        return pl.BlockSpec(shape, lambda p, i: (0,) * len(shape))

    d_hidden, d_down, d_up, d_task, d_slot = pl.pallas_call(
        generators,
        grid=(per, across),
        out_shape=(
            jax.ShapeDtypeStruct((tokens, width), bf),
            jax.ShapeDtypeStruct((cond_width, span), f32),
            jax.ShapeDtypeStruct((cond_width, span), f32),
            jax.ShapeDtypeStruct((tasks, cond_width), f32),
            jax.ShapeDtypeStruct((blocks * experts, cond_width), f32),
        ),
        in_specs=[
            fixed(sections * blocks * combos, cond_width),
            pl.BlockSpec((sections, blocks, 2, combos, out_chunk), lambda p, i: (0, 0, 0, p, i)),
            here,
            fixed(blocks * experts, cond_width),
            fixed(sections, 8, cond_width),
        ],
        out_specs=(
            here, columns, columns, fixed(tasks, cond_width), fixed(blocks * experts, cond_width)
        ),
        compiler_params=pltpu.CompilerParams(vmem_limit_bytes=58 << 20),
        name="generators",
    )(cond_all, every, hidden.reshape(tokens, width), slot_sum, task_sums)
    return (
        d_hidden.reshape(1, micro, tok, width), d_down, d_up, d_task,
        d_slot.reshape(blocks, 1, experts, cond_width),
    )


def solution(mesh):
    placed = (
        P(None, "section", None, "dp", None),
        P(None, "dp", None),
        P(None, "section", None, "dp", None),
        P(None, "section", None, "dp", None),
        P(None, "dp"),
        P(),
        P(None, "section", None, None),
        P(None, "dp"),
        P(None, "dp"),
    )
    return jax.shard_map(
        on_device,
        mesh=mesh,
        in_specs=placed,
        out_specs=(
            P("section", None, "dp", None),
            P(None, "dp"),
            P(None, "dp"),
            P(),
            P(None, "section", None, None),
        ),
        check_vma=False,
    )
```
